32 devices in a mesh: gx: 4 (over z), gy: 8 (over y, x, core).
Axes of the slice: x: 2, y: 2, z: 4, core: 2. Of those that a mesh axis runs over, the one named last changes fastest.
Arguments:
- policy_logp: float32 [16, 512, 4096], P('gy', 'gx'), may hold values from -2 to 0
- anchor_logp: float32 [16, 512, 4096], P('gy', 'gx'), may hold values from -2 to 0
- lengths: int32 [16, 512], P('gy', 'gx'), may hold values from 512 to 4096
- rewards: int32 [16, 512], P('gy', 'gx'), may hold values from 0 to 8
- slot_prompt: int32 [16, 512], P('gy', 'gx'), may hold values from 0 to 511, as said below
Outputs:
- token_grad: float32 [16, 512, 4096], P(None, ('gx', 'gy'))
- sample_loss: float32 [16, 512], P(None, ('gx', 'gy'))
- advantage: float32 [16, 512], P(None, ('gx', 'gy'))
The draws below stay inside these ranges and needn't reach their ends.
Inputs may be any that keep to these rules, and one draw needn't show every extreme that they name: `slot_prompt`: for every member k and every aligned block of 128 slots, the slots of the block hold each prompt of the same block exactly once.
All inputs are finite; a program needn't handle non-finite values.
Results may differ from the reference program's by a relative error of at most 0.00002.
Values sent between devices are 32-bit elements; how exact they have to be, the bound alone decides.
A program may use at most 64 MiB of HBM per device.

```python
import jax
import jax.numpy as jnp

K = 16
LMAX = 4096
PROMPTS = 512
BLOCK = 128
SAMPLES = 8192
N_GX = 4


def draw_slot_prompt(key, part):
    subkeys = jax.random.split(jax.random.fold_in(key, 7), K * N_GX)
    shuffled = jax.vmap(lambda subkey: jax.random.permutation(subkey, BLOCK))(subkeys)
    shuffled = shuffled.astype(jnp.int32).reshape(K, N_GX, BLOCK)
    offsets = (jnp.arange(N_GX, dtype=jnp.int32) * BLOCK)[None, :, None]
    return (shuffled + offsets).reshape(K, PROMPTS).astype(jnp.int32)


def with_ends(values, stream_key, least, high):
    spot = [jax.random.randint(jax.random.fold_in(stream_key, axis), (), 0, length) for axis, length in enumerate(values.shape)]
    widest = values.shape.index(max(values.shape))
    neighbour = spot[:widest] + [(spot[widest] + 1) % values.shape[widest]] + spot[widest + 1:]
    return values.at[tuple(spot)].set(least).at[tuple(neighbour)].set(high)


def level_of(stream_key, shape, cuts, low, top_value):
    level, own = 1.0, jax.random.fold_in(stream_key, 6)
    for dim, shards_of in cuts:
        steps = jnp.exp(jax.random.uniform(jax.random.fold_in(own, dim), (shards_of,), jnp.float32, low / len(cuts), top_value / len(cuts)))
        level = level * jnp.repeat(steps, shape[dim] // shards_of).reshape([-1 if axis == dim else 1 for axis in range(len(shape))])
    return level


def setup_inputs(seed: int = 0) -> dict:
    key_list = jax.random.split(jax.random.key(seed), 6)
    policy_logp = jnp.clip(-2.0 + 2.0 * jax.random.uniform(key_list[0], (K, PROMPTS, LMAX), jnp.float32) ** level_of(key_list[0], (K, PROMPTS, LMAX), ((0, 8), (1, 4)), -0.2, 0.2), -2.0, 0.0)
    anchor_logp = jnp.clip(-2.0 + 2.0 * jax.random.uniform(key_list[1], (K, PROMPTS, LMAX), jnp.float32) ** level_of(key_list[1], (K, PROMPTS, LMAX), ((0, 8), (1, 4)), -0.2, 0.2), -2.0, 0.0)
    lengths = with_ends(jax.random.randint(key_list[2], (K, PROMPTS), LMAX // 8, LMAX + 1), jax.random.fold_in(key_list[2], 1), LMAX // 8, LMAX).astype(jnp.int32)
    rewards = with_ends(jax.random.randint(key_list[3], (K, PROMPTS), 0, 9), jax.random.fold_in(key_list[3], 1), 0, 8).astype(jnp.int32)
    slot_prompt = draw_slot_prompt(jax.random.fold_in(key_list[5], 71), 0)
    return dict(policy_logp=policy_logp, anchor_logp=anchor_logp, lengths=lengths, rewards=rewards, slot_prompt=slot_prompt)


kl_weight = 0.1


def reference(policy_logp, anchor_logp, lengths, rewards, slot_prompt):
    member_rows = jnp.arange(K, dtype=jnp.int32)[:, None]
    slot_ids = jnp.broadcast_to(jnp.arange(PROMPTS, dtype=jnp.int32)[None, :], (K, PROMPTS))
    inverse = jnp.zeros((K, PROMPTS), jnp.int32).at[member_rows, slot_prompt].set(slot_ids)
    policy = jnp.take_along_axis(policy_logp, inverse[:, :, None], axis=1)
    anchor = jnp.take_along_axis(anchor_logp, inverse[:, :, None], axis=1)
    seq_len = jnp.take_along_axis(lengths, inverse, axis=1)
    reward = jnp.take_along_axis(rewards, inverse, axis=1).astype(jnp.float32) * 0.25
    total = jnp.sum(reward, axis=0)
    advantage = (K * reward - total[None, :]) / (K - 1)
    ntok = jnp.sum(lengths).astype(jnp.float32)
    positions = jnp.arange(LMAX, dtype=jnp.int32)[None, None, :]
    valid = positions < seq_len[:, :, None]
    log_ratio = anchor - policy
    ratio = jnp.exp(log_ratio)
    token_term = -advantage[:, :, None] * policy + kl_weight * (ratio - log_ratio - 1.0)
    token_grad = jnp.where(valid, -advantage[:, :, None] + kl_weight * (1.0 - ratio), 0.0) * (SAMPLES * LMAX / ntok)
    sample_loss = jnp.sum(jnp.where(valid, token_term, 0.0), axis=2) * (SAMPLES / ntok)
    return token_grad, sample_loss, advantage
```

```python
import functools

import jax
import jax.numpy as jnp
from jax import lax
from jax.experimental import pallas as pl
from jax.experimental.pallas import tpu as pltpu
from jax.sharding import PartitionSpec as P

kl_weight = 0.1
LANES = 128
CHUNKS = 8
MESH = pl.DeviceIdType.MESH


def permuted(onehot, rows):
    high = rows.astype(jnp.bfloat16)
    rest = rows - high.astype(jnp.float32)
    middle = rest.astype(jnp.bfloat16)
    low = (rest - middle.astype(jnp.float32)).astype(jnp.bfloat16)
    dot = functools.partial(jnp.dot, preferred_element_type=jnp.float32)
    return dot(onehot, high) + dot(onehot, middle) + dot(onehot, low)


def folded(x):
    out = x[:, :LANES]
    for start in range(LANES, x.shape[1], LANES):
        out = out + x[:, start : start + LANES]
    return out


def exchange(
    n_gx, n_gy, policy_hbm, anchor_hbm, len_ref, reward_ref, prompt_ref,
    raw_hbm, heads_ref, tails_ref, ntok_ref,
    policy, anchor, sendbuf, onehot, len_col, sum_policy, sum_kl,
    heads_send, heads_recv, tails_send, tails_recv, counts,
    load_sem, send_sem, recv_sem, own_sem,
    head_send_sem, head_recv_sem, tail_send_sem, tail_recv_sem, count_send_sem, count_recv_sem,
):
    gx, gy = lax.axis_index("gx"), lax.axis_index("gy")
    members_dev, slots, seq = policy_hbm.shape
    part = slots // n_gy
    width = seq // CHUNKS

    barrier = pltpu.get_barrier_semaphore()
    for off in range(1, n_gy):
        pl.semaphore_signal(barrier, inc=1, device_id=(gx, lax.rem(gy + off, n_gy)), device_id_type=MESH)
    for off in range(1, n_gx):
        pl.semaphore_signal(barrier, inc=1, device_id=(lax.rem(gx + off, n_gx), gy), device_id_type=MESH)

    def loads(c):
        cols = pl.ds(pl.multiple_of(c * width, LANES), width)
        return (
            pltpu.make_async_copy(policy_hbm.at[:, :, cols], policy.at[c], load_sem.at[0, c]),
            pltpu.make_async_copy(anchor_hbm.at[:, :, cols], anchor.at[c], load_sem.at[1, c]),
        )

    for c in range(CHUNKS):
        for copy in loads(c):
            copy.start()

    sublane = lax.broadcasted_iota(jnp.int32, (slots, slots), 0)
    lane = lax.broadcasted_iota(jnp.int32, (slots, slots), 1)
    column = lax.broadcasted_iota(jnp.int32, (slots, LANES), 1)
    local_tokens = jnp.sum(len_ref[...].astype(jnp.float32))
    for m in range(members_dev):
        seq_len = len_ref[m : m + 1, :].astype(jnp.float32)
        reward = reward_ref[m : m + 1, :].astype(jnp.float32) * 0.25
        match = sublane == lax.rem(prompt_ref[m : m + 1, :], slots)
        onehot[m] = jnp.where(match, 1.0, 0.0).astype(jnp.bfloat16)
        len_col[m] = jnp.broadcast_to(
            jnp.sum(jnp.where(sublane == lane, seq_len, 0.0), axis=1, keepdims=True), (slots, LANES)
        )
        sorted_len = jnp.sum(jnp.where(match, seq_len, 0.0), axis=1, keepdims=True)
        sorted_reward = jnp.sum(jnp.where(match, reward, 0.0), axis=1, keepdims=True)
        heads_send[m] = jnp.where(
            column == 0, sorted_len, jnp.where(column == 1, sorted_reward, local_tokens)
        )
    sum_policy[...] = jnp.zeros_like(sum_policy)
    sum_kl[...] = jnp.zeros_like(sum_kl)

    def compute(c):
        for copy in loads(c):
            copy.wait()
        positions = (lax.broadcasted_iota(jnp.int32, (slots, width), 1) + c * width).astype(jnp.float32)
        for m in range(members_dev):
            pol = policy[c, m]
            log_ratio = anchor[c, m] - pol
            ratio = jnp.exp(log_ratio)
            valid = positions < len_col[m][:, :1]
            sum_policy[m] += folded(jnp.where(valid, pol, 0.0))
            sum_kl[m] += folded(jnp.where(valid, kl_weight * (ratio - log_ratio - 1.0), 0.0))
            sendbuf[c, m] = permuted(onehot[m], kl_weight * (1.0 - ratio))

    def rows_of(device):
        return pl.ds(pl.multiple_of(device * part, part), part)

    my_members = pl.ds(gy * members_dev, members_dev)

    def sends(c):
        cols = pl.ds(pl.multiple_of(c * width, LANES), width)
        copies = []
        for off in range(1, n_gy):
            peer = lax.rem(gy + off, n_gy)
            copies.append(
                pltpu.make_async_remote_copy(
                    src_ref=sendbuf.at[c, :, rows_of(peer), :],
                    dst_ref=raw_hbm.at[my_members, :, cols],
                    send_sem=send_sem.at[off - 1],
                    recv_sem=recv_sem.at[off - 1],
                    device_id=(gx, peer),
                    device_id_type=MESH,
                )
            )
        return copies

    def own(c):
        cols = pl.ds(pl.multiple_of(c * width, LANES), width)
        return pltpu.make_async_copy(
            sendbuf.at[c, :, rows_of(gy), :], raw_hbm.at[my_members, :, cols], own_sem.at[c]
        )

    def small_sends(src, dst, send, recv):
        copies = []
        for off in range(1, n_gy):
            peer = lax.rem(gy + off, n_gy)
            copies.append(
                pltpu.make_async_remote_copy(
                    src_ref=src.at[:, rows_of(peer), :],
                    dst_ref=dst.at[my_members],
                    send_sem=send.at[off - 1],
                    recv_sem=recv.at[off - 1],
                    device_id=(gx, peer),
                    device_id_type=MESH,
                )
            )
        copies.append(pltpu.make_async_copy(src.at[:, rows_of(gy), :], dst.at[my_members], send.at[n_gy - 1]))
        return copies

    def count_sends():
        return [
            pltpu.make_async_remote_copy(
                src_ref=counts.at[0],
                dst_ref=counts.at[off],
                send_sem=count_send_sem.at[off - 1],
                recv_sem=count_recv_sem.at[off - 1],
                device_id=(lax.rem(gx + off, n_gx), gy),
                device_id_type=MESH,
            )
            for off in range(1, n_gx)
        ]

    compute(0)
    pl.semaphore_wait(barrier, n_gy - 1 + n_gx - 1)
    head_copies = small_sends(heads_send, heads_recv, head_send_sem, head_recv_sem)
    for copy in head_copies:
        copy.start()

    def step(c, carry):
        for copy in sends(c - 1):
            copy.start()
        own(c - 1).start()
        compute(c)
        return carry

    lax.fori_loop(1, CHUNKS, step, 0)
    for copy in sends(CHUNKS - 1):
        copy.start()
    own(CHUNKS - 1).start()

    for m in range(members_dev):
        s1 = jnp.sum(permuted(onehot[m], sum_policy[m]), axis=1, keepdims=True)
        s2 = jnp.sum(permuted(onehot[m], sum_kl[m]), axis=1, keepdims=True)
        tails_send[m] = jnp.where(column == 0, s1, s2)
    for copy in head_copies:
        copy.wait()
    tokens = jnp.zeros((8, LANES), jnp.float32)
    for source in range(n_gy):
        tokens = tokens + heads_recv[source * members_dev, :8, :]
    counts[0] = tokens
    heads_ref[...] = heads_recv[...]
    tail_copies = small_sends(tails_send, tails_recv, tail_send_sem, tail_recv_sem)
    for copy in tail_copies:
        copy.start()
    count_copies = count_sends()
    for copy in count_copies:
        copy.start()
    for copy in count_copies:
        copy.wait()
    ntok_ref[...] = jnp.sum(counts[...], axis=0)
    for copy in tail_copies:
        copy.wait()
    tails_ref[...] = tails_recv[...]
    for c in range(CHUNKS):
        own(c).wait()
    for off in range(1, n_gy):
        source = lax.rem(gy + n_gy - off, n_gy)
        landed = raw_hbm.at[pl.ds(source * members_dev, members_dev)]
        pltpu.make_async_copy(landed, landed, recv_sem.at[off - 1]).wait()
        pltpu.make_async_copy(landed, landed, send_sem.at[off - 1]).wait()


def finish(samples, raw, heads, tails, ntok, grad, loss, adv):
    members, part = heads.shape[0], heads.shape[1]
    group, _, seq = raw.shape
    step = pl.program_id(0)
    tokens = ntok[:1, 2:3]
    total = jnp.sum(heads[...], axis=0)

    def advantage_of(head):
        return (members * head[:, :, 1:2] - total[None, :, 1:2]) / (members - 1)

    head = heads[pl.ds(step * group, group)]
    positions = lax.broadcasted_iota(jnp.int32, (group, part, seq), 2).astype(jnp.float32)
    scale = (samples * seq / tokens)[None]
    grad[...] = jnp.where(positions < head[:, :, :1], raw[...] - advantage_of(head), 0.0) * scale

    @pl.when(step == 0)
    def _():
        shape = (members, part, LANES)
        eye = lax.broadcasted_iota(jnp.int32, shape, 1) == lax.broadcasted_iota(jnp.int32, shape, 2)
        advantage = advantage_of(heads[...])
        value = (tails[:, :, 1:2] - advantage * tails[:, :, :1]) * (samples / tokens)[None]
        loss[...] = jnp.sum(jnp.where(eye, value, 0.0), axis=1)[:, :part]
        adv[...] = jnp.sum(jnp.where(eye, advantage, 0.0), axis=1)[:, :part]


def body(n_gx, n_gy, policy_logp, anchor_logp, lengths, rewards, slot_prompt):
    members_dev, slots, seq = policy_logp.shape
    members, part = members_dev * n_gy, slots // n_gy
    f32 = jnp.float32
    chunked = (CHUNKS, members_dev, slots, seq // CHUNKS)
    small = (members, part, LANES)
    any_spec = pl.BlockSpec(memory_space=pl.ANY)
    vmem_spec = pl.BlockSpec(memory_space=pltpu.VMEM)
    dma = pltpu.SemaphoreType.DMA
    raw, heads, tails, ntok = pl.pallas_call(
        functools.partial(exchange, n_gx, n_gy),
        out_shape=(
            jax.ShapeDtypeStruct((members, part, seq), f32),
            jax.ShapeDtypeStruct(small, f32),
            jax.ShapeDtypeStruct(small, f32),
            jax.ShapeDtypeStruct((8, LANES), f32),
        ),
        in_specs=[any_spec, any_spec, vmem_spec, vmem_spec, vmem_spec],
        out_specs=(any_spec, vmem_spec, vmem_spec, vmem_spec),
        scratch_shapes=[
            pltpu.VMEM(chunked, f32),
            pltpu.VMEM(chunked, f32),
            pltpu.VMEM(chunked, f32),
            pltpu.VMEM((members_dev, slots, slots), jnp.bfloat16),
            pltpu.VMEM((members_dev, slots, LANES), f32),
            pltpu.VMEM((members_dev, slots, LANES), f32),
            pltpu.VMEM((members_dev, slots, LANES), f32),
            pltpu.VMEM((members_dev, slots, LANES), f32),
            pltpu.VMEM(small, f32),
            pltpu.VMEM((members_dev, slots, LANES), f32),
            pltpu.VMEM(small, f32),
            pltpu.VMEM((n_gx, 8, LANES), f32),
            dma((2, CHUNKS)),
            dma((n_gy - 1,)),
            dma((n_gy - 1,)),
            dma((CHUNKS,)),
            dma((n_gy,)),
            dma((n_gy - 1,)),
            dma((n_gy,)),
            dma((n_gy - 1,)),
            dma((n_gx - 1,)),
            dma((n_gx - 1,)),
        ],
        compiler_params=pltpu.CompilerParams(collective_id=0, has_side_effects=True),
    )(policy_logp, anchor_logp, lengths, rewards, slot_prompt)
    group = 2
    samples = members * slots * n_gx
    block = pl.BlockSpec((group, part, seq), lambda i: (i, 0, 0))
    whole = lambda shape: pl.BlockSpec(shape, lambda i: (0,) * len(shape))
    return pl.pallas_call(
        functools.partial(finish, samples),
        grid=(members // group,),
        out_shape=(
            jax.ShapeDtypeStruct((members, part, seq), f32),
            jax.ShapeDtypeStruct((members, part), f32),
            jax.ShapeDtypeStruct((members, part), f32),
        ),
        in_specs=[block, whole(small), whole(small), whole((8, LANES))],
        out_specs=(block, whole((members, part)), whole((members, part))),
    )(raw, heads, tails, ntok)


def solution(mesh):
    placed = (P("gy", "gx", None), P("gy", "gx", None), P("gy", "gx"), P("gy", "gx"), P("gy", "gx"))
    return jax.shard_map(
        functools.partial(body, mesh.shape["gx"], mesh.shape["gy"]),
        mesh=mesh,
        in_specs=placed,
        out_specs=(P(None, ("gx", "gy"), None), P(None, ("gx", "gy")), P(None, ("gx", "gy"))),
        check_vma=False,
    )
```

```python
import functools

import jax
import jax.numpy as jnp
from jax import lax
from jax.experimental import pallas as pl
from jax.experimental.pallas import tpu as pltpu
from jax.sharding import PartitionSpec as P

kl_weight = 0.1
LANES = 128
CHUNKS = 8
MESH = pl.DeviceIdType.MESH


def partner(index, off, count):
    out, bit = index, 1
    while bit < count:
        if off & bit:
            out = out + bit - 2 * bit * lax.rem(index // bit, 2)
        bit *= 2
    return out


def offsets_by_distance(count):
    far = max(bin(off // 2).count("1") for off in range(1, count))
    near = [off for off in range(1, count) if bin(off // 2).count("1") < far]
    return near, [off for off in range(1, count) if off not in near]


def permuted(onehot, rows):
    high = rows.astype(jnp.bfloat16)
    rest = rows - high.astype(jnp.float32)
    middle = rest.astype(jnp.bfloat16)
    low = (rest - middle.astype(jnp.float32)).astype(jnp.bfloat16)
    dot = functools.partial(jnp.dot, preferred_element_type=jnp.float32)
    return dot(onehot, high) + dot(onehot, middle) + dot(onehot, low)


def folded(x):
    out = x[:, :LANES]
    for start in range(LANES, x.shape[1], LANES):
        out = out + x[:, start : start + LANES]
    return out


def exchange(
    n_gx, n_gy, policy_hbm, anchor_hbm, len_ref, reward_ref, prompt_ref,
    raw_hbm, heads_ref, tails_ref, ntok_ref,
    policy, anchor, sendbuf, onehot, len_col, sum_policy, sum_kl,
    heads_send, heads_recv, tails_send, tails_recv, counts,
    load_sem, send_sem, recv_sem, own_sem,
    head_send_sem, head_recv_sem, tail_send_sem, tail_recv_sem, count_send_sem, count_recv_sem,
):
    gx, gy = lax.axis_index("gx"), lax.axis_index("gy")
    members_dev, slots, seq = policy_hbm.shape
    part = slots // n_gy
    width = seq // CHUNKS

    near, far = offsets_by_distance(n_gy)
    barrier = pltpu.get_barrier_semaphore()
    for off in range(1, n_gy):
        pl.semaphore_signal(barrier, inc=1, device_id=(gx, partner(gy, off, n_gy)), device_id_type=MESH)
    for off in range(1, n_gx):
        pl.semaphore_signal(barrier, inc=1, device_id=(lax.rem(gx + off, n_gx), gy), device_id_type=MESH)

    def loads(c):
        cols = pl.ds(pl.multiple_of(c * width, LANES), width)
        return (
            pltpu.make_async_copy(policy_hbm.at[:, :, cols], policy.at[c], load_sem.at[0, c]),
            pltpu.make_async_copy(anchor_hbm.at[:, :, cols], anchor.at[c], load_sem.at[1, c]),
        )

    for c in range(CHUNKS):
        for copy in loads(c):
            copy.start()

    sublane = lax.broadcasted_iota(jnp.int32, (slots, slots), 0)
    lane = lax.broadcasted_iota(jnp.int32, (slots, slots), 1)
    column = lax.broadcasted_iota(jnp.int32, (slots, LANES), 1)
    local_tokens = jnp.sum(len_ref[...].astype(jnp.float32))
    for m in range(members_dev):
        seq_len = len_ref[m : m + 1, :].astype(jnp.float32)
        reward = reward_ref[m : m + 1, :].astype(jnp.float32) * 0.25
        match = sublane == lax.rem(prompt_ref[m : m + 1, :], slots)
        onehot[m] = jnp.where(match, 1.0, 0.0).astype(jnp.bfloat16)
        len_col[m] = jnp.broadcast_to(
            jnp.sum(jnp.where(sublane == lane, seq_len, 0.0), axis=1, keepdims=True), (slots, LANES)
        )
        sorted_len = jnp.sum(jnp.where(match, seq_len, 0.0), axis=1, keepdims=True)
        sorted_reward = jnp.sum(jnp.where(match, reward, 0.0), axis=1, keepdims=True)
        heads_send[m] = jnp.where(
            column == 0, sorted_len, jnp.where(column == 1, sorted_reward, local_tokens)
        )
    sum_policy[...] = jnp.zeros_like(sum_policy)
    sum_kl[...] = jnp.zeros_like(sum_kl)

    def compute(c):
        for copy in loads(c):
            copy.wait()
        positions = (lax.broadcasted_iota(jnp.int32, (slots, width), 1) + c * width).astype(jnp.float32)
        for m in range(members_dev):
            pol = policy[c, m]
            log_ratio = anchor[c, m] - pol
            ratio = jnp.exp(log_ratio)
            valid = positions < len_col[m][:, :1]
            sum_policy[m] += folded(jnp.where(valid, pol, 0.0))
            sum_kl[m] += folded(jnp.where(valid, kl_weight * (ratio - log_ratio - 1.0), 0.0))
            sendbuf[c, m] = permuted(onehot[m], kl_weight * (1.0 - ratio))

    def rows_of(device):
        return pl.ds(pl.multiple_of(device * part, part), part)

    my_members = pl.ds(gy * members_dev, members_dev)

    def sends(c, offs):
        cols = pl.ds(pl.multiple_of(c * width, LANES), width)
        copies = []
        for off in offs:
            peer = partner(gy, off, n_gy)
            copies.append(
                pltpu.make_async_remote_copy(
                    src_ref=sendbuf.at[c, :, rows_of(peer), :],
                    dst_ref=raw_hbm.at[my_members, :, cols],
                    send_sem=send_sem.at[off - 1],
                    recv_sem=recv_sem.at[off - 1],
                    device_id=(gx, peer),
                    device_id_type=MESH,
                )
            )
        return copies

    def own(c):
        cols = pl.ds(pl.multiple_of(c * width, LANES), width)
        return pltpu.make_async_copy(
            sendbuf.at[c, :, rows_of(gy), :], raw_hbm.at[my_members, :, cols], own_sem.at[c]
        )

    def small_sends(src, dst, send, recv):
        copies = []
        for off in range(1, n_gy):
            peer = partner(gy, off, n_gy)
            copies.append(
                pltpu.make_async_remote_copy(
                    src_ref=src.at[:, rows_of(peer), :],
                    dst_ref=dst.at[my_members],
                    send_sem=send.at[off - 1],
                    recv_sem=recv.at[off - 1],
                    device_id=(gx, peer),
                    device_id_type=MESH,
                )
            )
        copies.append(pltpu.make_async_copy(src.at[:, rows_of(gy), :], dst.at[my_members], send.at[n_gy - 1]))
        return copies

    def count_sends():
        return [
            pltpu.make_async_remote_copy(
                src_ref=counts.at[0],
                dst_ref=counts.at[off],
                send_sem=count_send_sem.at[off - 1],
                recv_sem=count_recv_sem.at[off - 1],
                device_id=(lax.rem(gx + off, n_gx), gy),
                device_id_type=MESH,
            )
            for off in range(1, n_gx)
        ]

    compute(0)
    pl.semaphore_wait(barrier, n_gy - 1 + n_gx - 1)
    head_copies = small_sends(heads_send, heads_recv, head_send_sem, head_recv_sem)
    for copy in head_copies:
        copy.start()

    def step(c, carry):
        for copy in sends(c - 1, near):
            copy.start()
        own(c - 1).start()
        compute(c)
        return carry

    lax.fori_loop(1, CHUNKS, step, 0)
    for copy in sends(CHUNKS - 1, near):
        copy.start()

    def far_step(c, carry):
        for copy in sends(c, far):
            copy.start()
        return carry

    lax.fori_loop(0, CHUNKS, far_step, 0)
    own(CHUNKS - 1).start()

    for m in range(members_dev):
        s1 = jnp.sum(permuted(onehot[m], sum_policy[m]), axis=1, keepdims=True)
        s2 = jnp.sum(permuted(onehot[m], sum_kl[m]), axis=1, keepdims=True)
        tails_send[m] = jnp.where(column == 0, s1, s2)
    for copy in head_copies:
        copy.wait()
    tokens = jnp.zeros((8, LANES), jnp.float32)
    for source in range(n_gy):
        tokens = tokens + heads_recv[source * members_dev, :8, :]
    counts[0] = tokens
    heads_ref[...] = heads_recv[...]
    tail_copies = small_sends(tails_send, tails_recv, tail_send_sem, tail_recv_sem)
    for copy in tail_copies:
        copy.start()
    count_copies = count_sends()
    for copy in count_copies:
        copy.start()
    for copy in count_copies:
        copy.wait()
    ntok_ref[...] = jnp.sum(counts[...], axis=0)
    for copy in tail_copies:
        copy.wait()
    tails_ref[...] = tails_recv[...]
    for c in range(CHUNKS):
        own(c).wait()
    for off in range(1, n_gy):
        source = partner(gy, off, n_gy)
        landed = raw_hbm.at[pl.ds(source * members_dev, members_dev)]
        pltpu.make_async_copy(landed, landed, recv_sem.at[off - 1]).wait()
        pltpu.make_async_copy(landed, landed, send_sem.at[off - 1]).wait()


def finish(samples, raw, heads, tails, ntok, grad, loss, adv):
    members, part = heads.shape[0], heads.shape[1]
    group, _, seq = grad.shape
    step = pl.program_id(0)
    tokens = ntok[:1, 2:3]
    total = jnp.sum(heads[...], axis=0)

    def advantage_of(head):
        return (members * head[:, :, 1:2] - total[None, :, 1:2]) / (members - 1)

    head = heads[pl.ds(step * group, group)]
    positions = lax.broadcasted_iota(jnp.int32, (group, part, seq), 2).astype(jnp.float32)
    scale = (samples * seq / tokens)[None]
    grad[...] = jnp.where(positions < head[:, :, :1], raw[pl.ds(step * group, group)] - advantage_of(head), 0.0) * scale

    @pl.when(step == 0)
    def _():
        shape = (members, part, LANES)
        eye = lax.broadcasted_iota(jnp.int32, shape, 1) == lax.broadcasted_iota(jnp.int32, shape, 2)
        advantage = advantage_of(heads[...])
        value = (tails[:, :, 1:2] - advantage * tails[:, :, :1]) * (samples / tokens)[None]
        loss[...] = jnp.sum(jnp.where(eye, value, 0.0), axis=1)[:, :part]
        adv[...] = jnp.sum(jnp.where(eye, advantage, 0.0), axis=1)[:, :part]


def body(n_gx, n_gy, policy_logp, anchor_logp, lengths, rewards, slot_prompt):
    members_dev, slots, seq = policy_logp.shape
    members, part = members_dev * n_gy, slots // n_gy
    f32 = jnp.float32
    chunked = (CHUNKS, members_dev, slots, seq // CHUNKS)
    small = (members, part, LANES)
    hbm_spec = pl.BlockSpec(memory_space=pltpu.HBM)
    any_spec = pl.BlockSpec(memory_space=pl.ANY)
    vmem_spec = pl.BlockSpec(memory_space=pltpu.VMEM)
    dma = pltpu.SemaphoreType.DMA
    raw, heads, tails, ntok = pl.pallas_call(
        functools.partial(exchange, n_gx, n_gy),
        out_shape=(
            pltpu.VMEM((members, part, seq), f32),
            pltpu.VMEM(small, f32),
            pltpu.VMEM(small, f32),
            pltpu.VMEM((8, LANES), f32),
        ),
        in_specs=[hbm_spec, hbm_spec, vmem_spec, vmem_spec, vmem_spec],
        out_specs=(vmem_spec, vmem_spec, vmem_spec, vmem_spec),
        scratch_shapes=[
            pltpu.VMEM(chunked, f32),
            pltpu.VMEM(chunked, f32),
            pltpu.VMEM(chunked, f32),
            pltpu.VMEM((members_dev, slots, slots), jnp.bfloat16),
            pltpu.VMEM((members_dev, slots, LANES), f32),
            pltpu.VMEM((members_dev, slots, LANES), f32),
            pltpu.VMEM((members_dev, slots, LANES), f32),
            pltpu.VMEM((members_dev, slots, LANES), f32),
            pltpu.VMEM(small, f32),
            pltpu.VMEM((members_dev, slots, LANES), f32),
            pltpu.VMEM(small, f32),
            pltpu.VMEM((n_gx, 8, LANES), f32),
            dma((2, CHUNKS)),
            dma((n_gy - 1,)),
            dma((n_gy - 1,)),
            dma((CHUNKS,)),
            dma((n_gy,)),
            dma((n_gy - 1,)),
            dma((n_gy,)),
            dma((n_gy - 1,)),
            dma((n_gx - 1,)),
            dma((n_gx - 1,)),
        ],
        compiler_params=pltpu.CompilerParams(collective_id=0, has_side_effects=True, vmem_limit_bytes=56 * 2**20),
    )(policy_logp, anchor_logp, lengths, rewards, slot_prompt)
    group = 4
    samples = members * slots * n_gx
    block = pl.BlockSpec((group, part, seq), lambda i: (i, 0, 0))
    whole = lambda shape: pl.BlockSpec(shape, lambda i: (0,) * len(shape))
    return pl.pallas_call(
        functools.partial(finish, samples),
        grid=(members // group,),
        out_shape=(
            jax.ShapeDtypeStruct((members, part, seq), f32),
            jax.ShapeDtypeStruct((members, part), f32),
            jax.ShapeDtypeStruct((members, part), f32),
        ),
        in_specs=[vmem_spec] * 4,
        out_specs=(block, whole((members, part)), whole((members, part))),
        compiler_params=pltpu.CompilerParams(vmem_limit_bytes=32 * 2**20),
    )(raw, heads, tails, ntok)


def solution(mesh):
    placed = (P("gy", "gx", None), P("gy", "gx", None), P("gy", "gx"), P("gy", "gx"), P("gy", "gx"))
    return jax.shard_map(
        functools.partial(body, mesh.shape["gx"], mesh.shape["gy"]),
        mesh=mesh,
        in_specs=placed,
        out_specs=(P(None, ("gx", "gy"), None), P(None, ("gx", "gy")), P(None, ("gx", "gy"))),
        check_vma=False,
    )
```

```python
import functools

import jax
import jax.numpy as jnp
from jax import lax
from jax.experimental import pallas as pl
from jax.experimental.pallas import tpu as pltpu
from jax.sharding import PartitionSpec as P

kl_weight = 0.1
LANES = 128
CHUNKS = 8
MESH = pl.DeviceIdType.MESH


def partner(index, off, count):
    out, bit = index, 1
    while bit < count:
        if off & bit:
            out = out + bit - 2 * bit * lax.rem(index // bit, 2)
        bit *= 2
    return out


def offsets_by_distance(count):
    far = max(bin(off // 2).count("1") for off in range(1, count))
    near = [off for off in range(1, count) if bin(off // 2).count("1") < far]
    return near, [off for off in range(1, count) if off not in near]


def permuted(onehot, rows):
    high = rows.astype(jnp.bfloat16)
    rest = rows - high.astype(jnp.float32)
    middle = rest.astype(jnp.bfloat16)
    low = (rest - middle.astype(jnp.float32)).astype(jnp.bfloat16)
    dot = functools.partial(jnp.dot, preferred_element_type=jnp.float32)
    return dot(onehot, high) + dot(onehot, middle) + dot(onehot, low)


def folded(x):
    out = x[:, :LANES]
    for start in range(LANES, x.shape[1], LANES):
        out = out + x[:, start : start + LANES]
    return out


def exchange(
    n_gx, n_gy, policy_hbm, anchor_hbm, len_ref, reward_ref, prompt_ref,
    raw_hbm, heads_ref, tails_ref, ntok_ref,
    policy, anchor, sendbuf, onehot, len_col, sum_policy, sum_kl,
    heads_send, heads_recv, tails_send, tails_recv, counts,
    load_sem, send_sem, recv_sem, own_sem,
    head_send_sem, head_recv_sem, tail_send_sem, tail_recv_sem, count_send_sem, count_recv_sem,
):
    gx, gy = lax.axis_index("gx"), lax.axis_index("gy")
    members_dev, slots, seq = policy_hbm.shape
    part = slots // n_gy
    width = seq // CHUNKS

    near, far = offsets_by_distance(n_gy)
    barrier = pltpu.get_barrier_semaphore()
    for off in range(1, n_gy):
        pl.semaphore_signal(barrier, inc=1, device_id=(gx, partner(gy, off, n_gy)), device_id_type=MESH)
    for off in range(1, n_gx):
        pl.semaphore_signal(barrier, inc=1, device_id=(lax.rem(gx + off, n_gx), gy), device_id_type=MESH)

    def loads(c):
        cols = pl.ds(pl.multiple_of(c * width, LANES), width)
        return (
            pltpu.make_async_copy(policy_hbm.at[:, :, cols], policy.at[c], load_sem.at[0, c]),
            pltpu.make_async_copy(anchor_hbm.at[:, :, cols], anchor.at[c], load_sem.at[1, c]),
        )

    for c in range(CHUNKS):
        for copy in loads(c):
            copy.start()

    sublane = lax.broadcasted_iota(jnp.int32, (slots, slots), 0)
    lane = lax.broadcasted_iota(jnp.int32, (slots, slots), 1)
    column = lax.broadcasted_iota(jnp.int32, (slots, LANES), 1)
    local_tokens = jnp.sum(len_ref[...].astype(jnp.float32))
    for m in range(members_dev):
        seq_len = len_ref[m : m + 1, :].astype(jnp.float32)
        reward = reward_ref[m : m + 1, :].astype(jnp.float32) * 0.25
        match = sublane == lax.rem(prompt_ref[m : m + 1, :], slots)
        onehot[m] = jnp.where(match, 1.0, 0.0).astype(jnp.bfloat16)
        len_col[m] = jnp.broadcast_to(
            jnp.sum(jnp.where(sublane == lane, seq_len, 0.0), axis=1, keepdims=True), (slots, LANES)
        )
        sorted_len = jnp.sum(jnp.where(match, seq_len, 0.0), axis=1, keepdims=True)
        sorted_reward = jnp.sum(jnp.where(match, reward, 0.0), axis=1, keepdims=True)
        heads_send[m] = jnp.where(
            column == 0, sorted_len, jnp.where(column == 1, sorted_reward, local_tokens)
        )
    sum_policy[...] = jnp.zeros_like(sum_policy)
    sum_kl[...] = jnp.zeros_like(sum_kl)

    def compute(c):
        for copy in loads(c):
            copy.wait()
        positions = (lax.broadcasted_iota(jnp.int32, (slots, width), 1) + c * width).astype(jnp.float32)
        for m in range(members_dev):
            pol = policy[c, m]
            log_ratio = anchor[c, m] - pol
            ratio = jnp.exp(log_ratio)
            valid = positions < len_col[m][:, :1]
            sum_policy[m] += folded(jnp.where(valid, pol, 0.0))
            sum_kl[m] += folded(jnp.where(valid, kl_weight * (ratio - log_ratio - 1.0), 0.0))
            sendbuf[c, m] = permuted(onehot[m], kl_weight * (1.0 - ratio))

    def rows_of(device):
        return pl.ds(pl.multiple_of(device * part, part), part)

    my_members = pl.ds(gy * members_dev, members_dev)

    def sends(c, offs):
        cols = pl.ds(pl.multiple_of(c * width, LANES), width)
        copies = []
        for off in offs:
            peer = partner(gy, off, n_gy)
            copies.append(
                pltpu.make_async_remote_copy(
                    src_ref=sendbuf.at[c, :, rows_of(peer), :],
                    dst_ref=raw_hbm.at[my_members, :, cols],
                    send_sem=send_sem.at[off - 1],
                    recv_sem=recv_sem.at[off - 1],
                    device_id=(gx, peer),
                    device_id_type=MESH,
                )
            )
        return copies

    def own(c):
        cols = pl.ds(pl.multiple_of(c * width, LANES), width)
        return pltpu.make_async_copy(
            sendbuf.at[c, :, rows_of(gy), :], raw_hbm.at[my_members, :, cols], own_sem.at[c]
        )

    def small_sends(src, dst, send, recv):
        copies = []
        for off in range(1, n_gy):
            peer = partner(gy, off, n_gy)
            copies.append(
                pltpu.make_async_remote_copy(
                    src_ref=src.at[:, rows_of(peer), :],
                    dst_ref=dst.at[my_members],
                    send_sem=send.at[off - 1],
                    recv_sem=recv.at[off - 1],
                    device_id=(gx, peer),
                    device_id_type=MESH,
                )
            )
        copies.append(pltpu.make_async_copy(src.at[:, rows_of(gy), :], dst.at[my_members], send.at[n_gy - 1]))
        return copies

    def count_sends():
        return [
            pltpu.make_async_remote_copy(
                src_ref=counts.at[0],
                dst_ref=counts.at[off],
                send_sem=count_send_sem.at[off - 1],
                recv_sem=count_recv_sem.at[off - 1],
                device_id=(lax.rem(gx + off, n_gx), gy),
                device_id_type=MESH,
            )
            for off in range(1, n_gx)
        ]

    compute(0)
    pl.semaphore_wait(barrier, n_gy - 1 + n_gx - 1)
    head_copies = small_sends(heads_send, heads_recv, head_send_sem, head_recv_sem)
    for copy in head_copies:
        copy.start()

    def step(c, carry):
        for copy in sends(c - 1, near):
            copy.start()
        own(c - 1).start()
        compute(c)
        return carry

    lax.fori_loop(1, CHUNKS, step, 0)
    for copy in sends(CHUNKS - 1, near):
        copy.start()

    def far_step(c, carry):
        for copy in sends(c, far):
            copy.start()
        return carry

    lax.fori_loop(0, CHUNKS, far_step, 0)
    own(CHUNKS - 1).start()

    for m in range(members_dev):
        s1 = jnp.sum(permuted(onehot[m], sum_policy[m]), axis=1, keepdims=True)
        s2 = jnp.sum(permuted(onehot[m], sum_kl[m]), axis=1, keepdims=True)
        tails_send[m] = jnp.where(column == 0, s1, s2)
    for copy in head_copies:
        copy.wait()
    tokens = jnp.zeros((8, LANES), jnp.float32)
    for source in range(n_gy):
        tokens = tokens + heads_recv[source * members_dev, :8, :]
    counts[0] = tokens
    heads_ref[...] = heads_recv[...]
    tail_copies = small_sends(tails_send, tails_recv, tail_send_sem, tail_recv_sem)
    for copy in tail_copies:
        copy.start()
    count_copies = count_sends()
    for copy in count_copies:
        copy.start()
    for copy in count_copies:
        copy.wait()
    ntok_ref[...] = jnp.sum(counts[...], axis=0)
    for copy in tail_copies:
        copy.wait()
    tails_ref[...] = tails_recv[...]
    for c in range(CHUNKS):
        own(c).wait()
    for off in range(1, n_gy):
        source = partner(gy, off, n_gy)
        landed = raw_hbm.at[pl.ds(source * members_dev, members_dev)]
        pltpu.make_async_copy(landed, landed, recv_sem.at[off - 1]).wait()
        pltpu.make_async_copy(landed, landed, send_sem.at[off - 1]).wait()


def finish(samples, raw, heads, tails, ntok, grad, loss, adv, done, done_sem):
    members, part, seq = raw.shape
    tokens = ntok[:1, 2:3]
    total = jnp.sum(heads[...], axis=0)
    advantage = (members * heads[:, :, 1:2] - total[None, :, 1:2]) / (members - 1)
    positions = lax.broadcasted_iota(jnp.int32, (part, seq), 1).astype(jnp.float32)
    scale = samples * seq / tokens

    def store(k):
        return pltpu.make_async_copy(done.at[k], grad.at[k], done_sem.at[k])

    for k in range(members):
        done[k] = jnp.where(positions < heads[k, :, :1], raw[k] - advantage[k], 0.0) * scale
        if k > 0:
            store(k - 1).start()
    shape = (members, part, LANES)
    eye = lax.broadcasted_iota(jnp.int32, shape, 1) == lax.broadcasted_iota(jnp.int32, shape, 2)
    store(members - 1).start()
    value = (tails[:, :, 1:2] - advantage * tails[:, :, :1]) * (samples / tokens)[None]
    loss[...] = jnp.sum(jnp.where(eye, value, 0.0), axis=1)[:, :part]
    adv[...] = jnp.sum(jnp.where(eye, advantage, 0.0), axis=1)[:, :part]
    for k in range(members):
        store(k).wait()


def body(n_gx, n_gy, policy_logp, anchor_logp, lengths, rewards, slot_prompt):
    members_dev, slots, seq = policy_logp.shape
    members, part = members_dev * n_gy, slots // n_gy
    f32 = jnp.float32
    chunked = (CHUNKS, members_dev, slots, seq // CHUNKS)
    small = (members, part, LANES)
    hbm_spec = pl.BlockSpec(memory_space=pltpu.HBM)
    vmem_spec = pl.BlockSpec(memory_space=pltpu.VMEM)
    dma = pltpu.SemaphoreType.DMA
    raw, heads, tails, ntok = pl.pallas_call(
        functools.partial(exchange, n_gx, n_gy),
        out_shape=(
            pltpu.VMEM((members, part, seq), f32),
            pltpu.VMEM(small, f32),
            pltpu.VMEM(small, f32),
            pltpu.VMEM((8, LANES), f32),
        ),
        in_specs=[hbm_spec, hbm_spec, vmem_spec, vmem_spec, vmem_spec],
        out_specs=(vmem_spec, vmem_spec, vmem_spec, vmem_spec),
        scratch_shapes=[
            pltpu.VMEM(chunked, f32),
            pltpu.VMEM(chunked, f32),
            pltpu.VMEM(chunked, f32),
            pltpu.VMEM((members_dev, slots, slots), jnp.bfloat16),
            pltpu.VMEM((members_dev, slots, LANES), f32),
            pltpu.VMEM((members_dev, slots, LANES), f32),
            pltpu.VMEM((members_dev, slots, LANES), f32),
            pltpu.VMEM((members_dev, slots, LANES), f32),
            pltpu.VMEM(small, f32),
            pltpu.VMEM((members_dev, slots, LANES), f32),
            pltpu.VMEM(small, f32),
            pltpu.VMEM((n_gx, 8, LANES), f32),
            dma((2, CHUNKS)),
            dma((n_gy - 1,)),
            dma((n_gy - 1,)),
            dma((CHUNKS,)),
            dma((n_gy,)),
            dma((n_gy - 1,)),
            dma((n_gy,)),
            dma((n_gy - 1,)),
            dma((n_gx - 1,)),
            dma((n_gx - 1,)),
        ],
        compiler_params=pltpu.CompilerParams(collective_id=0, has_side_effects=True, vmem_limit_bytes=56 * 2**20),
    )(policy_logp, anchor_logp, lengths, rewards, slot_prompt)
    samples = members * slots * n_gx
    return pl.pallas_call(
        functools.partial(finish, samples),
        out_shape=(
            jax.ShapeDtypeStruct((members, part, seq), f32),
            jax.ShapeDtypeStruct((members, part), f32),
            jax.ShapeDtypeStruct((members, part), f32),
        ),
        in_specs=[vmem_spec] * 4,
        out_specs=(hbm_spec, vmem_spec, vmem_spec),
        scratch_shapes=[pltpu.VMEM((members, part, seq), f32), dma((members,))],
        compiler_params=pltpu.CompilerParams(vmem_limit_bytes=32 * 2**20),
    )(raw, heads, tails, ntok)


def solution(mesh):
    placed = (P("gy", "gx", None), P("gy", "gx", None), P("gy", "gx"), P("gy", "gx"), P("gy", "gx"))
    return jax.shard_map(
        functools.partial(body, mesh.shape["gx"], mesh.shape["gy"]),
        mesh=mesh,
        in_specs=placed,
        out_specs=(P(None, ("gx", "gy"), None), P(None, ("gx", "gy")), P(None, ("gx", "gy"))),
        check_vma=False,
    )
```
